32 devices in a mesh: part: 1 (over z), tp: 4 (over y), ep: 8 (over x, core).
Axes of the slice: x: 4, y: 4, z: 1, core: 2. Of those that a mesh axis runs over, the one named last changes fastest.
The devices are a block of a 4x4x8 slice.
Arguments:
- x_in: bfloat16 [64, 1024, 768], P(('part', 'ep'))
- idx_first: int32 [64, 1024], P(('part', 'ep'))
- idx_second: int32 [64, 1024], P(('part', 'ep'))
- rel_bias: float32 [2, 12, 1024], P(None, 'tp')
- norm_gain: float32 [4, 768], replicated
- attn_qkv: bfloat16 [2, 3, 768, 768], P(None, None, None, 'tp')
- attn_out: bfloat16 [2, 768, 768], P(None, 'tp')
- gate_w: float32 [768, 64], replicated
- expert_w0: bfloat16 [64, 768, 3072], P('ep', None, 'tp')
- expert_w1: bfloat16 [64, 768, 3072], P('ep', None, 'tp')
- expert_down: bfloat16 [64, 3072, 768], P('ep', 'tp')
- dense_w0: bfloat16 [768, 3072], P(None, 'tp')
- dense_w1: bfloat16 [768, 3072], P(None, 'tp')
- dense_down: bfloat16 [3072, 768], P('tp')
Outputs:
- output: bfloat16 [64, 1024, 768], P(('part', 'ep'))
All inputs are finite; a program needn't handle non-finite values.
Results may differ from the reference program's by a relative error of at most 0.02.
Values are sent between devices in bfloat16 or wider.
A program may use at most 768 MiB of HBM per device.

```python
import functools
import jax
import jax.numpy as jnp
from jax import lax

GROUPS = 8
SEQS_DEV = 8
SEQ = 1024
D = 768
FF = 3072
HEADS = 12
EXPERTS = 64


def draw_routing(key):
    k_cover, k_draw, k_shift = jax.random.split(key, 3)
    group_tokens = SEQS_DEV * SEQ
    favoured = max(1, EXPERTS // 8)
    cover = jax.vmap(lambda sub_key: jax.random.permutation(sub_key, EXPERTS))(jax.random.split(k_cover, GROUPS))
    raw_draw = jax.random.randint(k_draw, (GROUPS, group_tokens - EXPERTS), 0, 2 * EXPERTS, dtype=jnp.int32)
    skewed = jnp.where(raw_draw < EXPERTS, raw_draw, ((raw_draw - EXPERTS) % favoured) * (EXPERTS // favoured))
    first = jnp.concatenate([cover.astype(jnp.int32), skewed], axis=1)
    shift = jax.random.randint(k_shift, (GROUPS, group_tokens), 1, EXPERTS, dtype=jnp.int32)
    second = (first + shift) % EXPERTS
    return first.reshape(GROUPS * SEQS_DEV, SEQ), second.reshape(GROUPS * SEQS_DEV, SEQ)


def setup_inputs(seed: int = 0, part: int = 0) -> dict:
    key = jax.random.key(seed)
    shared = jax.random.split(key, 11)
    local = jax.random.split(jax.random.fold_in(key, part), 2)
    idx_first, idx_second = draw_routing(local[1])
    out_gain = max(1.0, (SEQ / 64) ** 0.5)
    qkv_gain = jnp.array([1.2, 1.2, 1.0], jnp.float32).reshape(1, 3, 1, 1)

    def normal(sub_key, shape, scale):
        return jax.random.normal(sub_key, shape, jnp.float32) * scale

    return {
        "x_in": normal(local[0], (GROUPS * SEQS_DEV, SEQ, D), 1.0).astype(jnp.bfloat16),
        "idx_first": idx_first,
        "idx_second": idx_second,
        "rel_bias": normal(shared[0], (2, HEADS, SEQ), 1.0),
        "norm_gain": jax.random.uniform(shared[1], (4, D), jnp.float32, 0.5, 1.5),
        "attn_qkv": (normal(shared[2], (2, 3, D, D), D ** -0.5) * qkv_gain).astype(jnp.bfloat16),
        "attn_out": normal(shared[3], (2, D, D), out_gain * D ** -0.5).astype(jnp.bfloat16),
        "gate_w": normal(shared[4], (D, EXPERTS), 2.0 * D ** -0.5),
        "expert_w0": normal(shared[5], (EXPERTS, D, FF), D ** -0.5).astype(jnp.bfloat16),
        "expert_w1": normal(shared[6], (EXPERTS, D, FF), D ** -0.5).astype(jnp.bfloat16),
        "expert_down": normal(shared[7], (EXPERTS, FF, D), FF ** -0.5).astype(jnp.bfloat16),
        "dense_w0": normal(shared[8], (D, FF), D ** -0.5).astype(jnp.bfloat16),
        "dense_w1": normal(shared[9], (D, FF), D ** -0.5).astype(jnp.bfloat16),
        "dense_down": normal(shared[10], (FF, D), FF ** -0.5).astype(jnp.bfloat16),
    }


def rms_norm(hidden, gain):
    wide = hidden.astype(jnp.float32)
    scale = lax.rsqrt(jnp.mean(wide * wide, axis=-1, keepdims=True) + 1e-6)
    return (wide * scale * gain).astype(jnp.bfloat16)


def add_residual(base, branch):
    return (base.astype(jnp.float32) + branch.astype(jnp.float32)).astype(jnp.bfloat16)


def causal_bias(rel_table, row_start, rows):
    heads, length = rel_table.shape
    pattern = jnp.concatenate([rel_table[:, :1], jnp.zeros((heads, length), rel_table.dtype), rel_table[:, :0:-1]], axis=1)
    pattern = jnp.roll(pattern, row_start, axis=1)
    flat = jnp.tile(pattern, (1, rows))[:, : rows * (2 * length - 1)]
    table = flat.reshape(heads, rows, 2 * length - 1)[:, :, :length]
    later = jnp.arange(length)[None, :] > (row_start + jnp.arange(rows))[:, None]
    return jnp.where(later[None], -1e30, table)


def route(idx_first, idx_second, gate_probs):
    group_tokens, experts = gate_probs.shape
    capacity = (2 * group_tokens + experts - 1) // experts
    expert_ids = jnp.arange(experts, dtype=jnp.int32)
    hot_first = (idx_first[:, None] == expert_ids).astype(jnp.int32)
    hot_second = (idx_second[:, None] == expert_ids).astype(jnp.int32)
    pos_first = jnp.sum((jnp.cumsum(hot_first, axis=0) - 1) * hot_first, axis=1)
    first_count = jnp.sum(hot_first, axis=0)
    pos_second = jnp.sum((jnp.cumsum(hot_second, axis=0) - 1 + first_count[None, :]) * hot_second, axis=1)
    gate_first = jnp.sum(jnp.where(hot_first == 1, gate_probs, 0.0), axis=1)
    gate_second = jnp.sum(jnp.where(hot_second == 1, gate_probs, 0.0), axis=1)
    total = gate_first + gate_second
    empty = experts * capacity
    slot_first = jnp.where(pos_first < capacity, idx_first * capacity + pos_first, empty)
    slot_second = jnp.where(pos_second < capacity, idx_second * capacity + pos_second, empty)
    return slot_first, slot_second, gate_first / total, gate_second / total


def dispatch(h_flat, slot_first, slot_second, experts):
    group_tokens = h_flat.shape[0]
    capacity = (2 * group_tokens + experts - 1) // experts
    token_ids = jnp.arange(group_tokens, dtype=jnp.int32)
    slot_token = jnp.full((experts * capacity,), group_tokens, jnp.int32)
    slot_token = slot_token.at[jnp.concatenate([slot_first, slot_second])].set(jnp.concatenate([token_ids, token_ids]), mode="drop")
    return jnp.take(h_flat, slot_token, axis=0, mode="fill", fill_value=0)


def combine(expert_rows, slot_first, slot_second, gate_first, gate_second):
    picked_first = jnp.take(expert_rows, slot_first, axis=0, mode="fill", fill_value=0).astype(jnp.float32)
    picked_second = jnp.take(expert_rows, slot_second, axis=0, mode="fill", fill_value=0).astype(jnp.float32)
    return gate_first[:, None] * picked_first + gate_second[:, None] * picked_second


def attention_layer(h_norm, qkv_w, out_w, rel_table):
    head_dim = D // HEADS
    bias = causal_bias(rel_table, 0, SEQ)
    qkv_wide = qkv_w.astype(jnp.float32)

    def one_seq(seq_norm):
        proj = jnp.einsum("ld,cdk->clk", seq_norm.astype(jnp.float32), qkv_wide).astype(jnp.bfloat16)
        heads_view = proj.reshape(3, SEQ, HEADS, head_dim).astype(jnp.float32)
        logits = jnp.einsum("qhe,khe->hqk", heads_view[0], heads_view[1]) * head_dim ** -0.5 + bias
        weights = jax.nn.softmax(logits, axis=-1).astype(jnp.bfloat16).astype(jnp.float32)
        context = jnp.einsum("hqk,khe->qhe", weights, heads_view[2]).astype(jnp.bfloat16)
        return jnp.dot(context.reshape(SEQ, D), out_w, preferred_element_type=jnp.float32).astype(jnp.bfloat16)

    return lax.map(one_seq, h_norm)


def moe_layer(h_norm, gate_w, idx_first, idx_second, expert_w0, expert_w1, expert_down):
    group_tokens = SEQS_DEV * SEQ
    tokens = h_norm.reshape(GROUPS, group_tokens, D)
    gate_probs = jax.nn.softmax(jnp.einsum("gtd,de->gte", tokens.astype(jnp.float32), gate_w), axis=-1)
    slot_first, slot_second, gate_first, gate_second = jax.vmap(route)(idx_first.reshape(GROUPS, group_tokens), idx_second.reshape(GROUPS, group_tokens), gate_probs)
    buffers = jax.vmap(functools.partial(dispatch, experts=EXPERTS))(tokens, slot_first, slot_second)
    capacity = buffers.shape[1] // EXPERTS
    expert_in = buffers.reshape(GROUPS, EXPERTS, capacity, D).transpose(1, 0, 2, 3).reshape(EXPERTS, GROUPS * capacity, D)

    def one_expert(operands):
        rows, first_w, second_w, down_w = operands
        hidden = (jax.nn.gelu(jnp.dot(rows, first_w, preferred_element_type=jnp.float32)) * jnp.dot(rows, second_w, preferred_element_type=jnp.float32)).astype(jnp.bfloat16)
        return jnp.dot(hidden, down_w, preferred_element_type=jnp.float32).astype(jnp.bfloat16)

    expert_out = lax.map(one_expert, (expert_in, expert_w0, expert_w1, expert_down))
    back = expert_out.reshape(EXPERTS, GROUPS, capacity, D).transpose(1, 0, 2, 3).reshape(GROUPS, EXPERTS * capacity, D)
    mixed = jax.vmap(combine)(back, slot_first, slot_second, gate_first, gate_second)
    return mixed.reshape(GROUPS * SEQS_DEV, SEQ, D)


def dense_layer(h_norm, first_w, second_w, down_w):
    def one_seq(seq_norm):
        hidden = (jax.nn.gelu(jnp.dot(seq_norm, first_w, preferred_element_type=jnp.float32)) * jnp.dot(seq_norm, second_w, preferred_element_type=jnp.float32)).astype(jnp.bfloat16)
        return jnp.dot(hidden, down_w, preferred_element_type=jnp.float32).astype(jnp.bfloat16)

    return lax.map(one_seq, h_norm)


def reference(x_in, idx_first, idx_second, rel_bias, norm_gain, attn_qkv, attn_out, gate_w, expert_w0, expert_w1, expert_down, dense_w0, dense_w1, dense_down):
    residual = add_residual(x_in, attention_layer(rms_norm(x_in, norm_gain[0]), attn_qkv[0], attn_out[0], rel_bias[0]))
    residual = add_residual(residual, moe_layer(rms_norm(residual, norm_gain[1]), gate_w, idx_first, idx_second, expert_w0, expert_w1, expert_down))
    residual = add_residual(residual, attention_layer(rms_norm(residual, norm_gain[2]), attn_qkv[1], attn_out[1], rel_bias[1]))
    return add_residual(residual, dense_layer(rms_norm(residual, norm_gain[3]), dense_w0, dense_w1, dense_down))
```

```python
import functools

import jax
import jax.numpy as jnp
from jax import lax
from jax.experimental import pallas as pl
from jax.experimental.pallas import tpu as pltpu
from jax.sharding import PartitionSpec as P


F32 = jnp.float32
BF16 = jnp.bfloat16
MASKED = -1e30
VMEM_BYTES = 60 << 20
COLS = 256


def dot(a, b):
    return jnp.dot(a, b, preferred_element_type=F32)


def norm_rows(wide, gain):
    scale = lax.rsqrt(jnp.mean(wide * wide, axis=-1, keepdims=True) + 1e-6)
    return (wide * scale * gain).astype(BF16)


def whole(*shape):
    return pl.BlockSpec(shape, lambda *_: (0,) * len(shape))


def params():
    return pltpu.CompilerParams(vmem_limit_bytes=VMEM_BYTES)


def cost(flops, nbytes):
    return pl.CostEstimate(flops=int(flops), bytes_accessed=int(nbytes), transcendentals=0)


def attention_body(heads, block, head_dim, has_add, *refs):
    x_ref, refs = refs[0], refs[1:]
    if has_add:
        add_ref, refs = refs[0], refs[1:]
    gain_in, gain_out, qkv_w, out_w, rel, res_ref, u_ref, src_s, acc_s, q_s, k_s, v_s, ctx_s, bias_s = refs
    step = pl.program_id(0)
    length = x_ref.shape[0]
    cols = heads * head_dim

    @pl.when(step == 0)
    def _():
        wide = x_ref[...].astype(F32)
        if has_add:
            wide = (wide + add_ref[...].astype(F32)).astype(BF16).astype(F32)
        res_ref[...] = wide.astype(BF16)
        src_s[...] = norm_rows(wide, gain_in[...])
        acc_s[...] = jnp.zeros_like(acc_s)

    source = src_s[...]
    weight = [qkv_w[0, :, n].reshape(source.shape[1], cols) for n in range(3)]
    q_s[...] = dot(source, weight[0]).astype(BF16) * jnp.bfloat16(head_dim ** -0.5)
    k_s[...] = dot(source, weight[1]).astype(BF16)
    v_s[...] = dot(source, weight[2]).astype(BF16)
    lane = lax.broadcasted_iota(jnp.int32, (block, cols), 1)
    span = length + block
    for head in range(heads):
        spread = jnp.broadcast_to(rel[head], (block, span))
        bias_s[head] = pltpu.roll(spread, span - block + 1, 1, stride=1, stride_axis=0)[:, :length]
    for part in range(length // block):
        keys = (part + 1) * block
        rows = pl.ds(part * block, block)
        context = jnp.zeros((block, cols), F32)
        for head in range(heads):
            mine = (lane >= head * head_dim) & (lane < (head + 1) * head_dim)
            query = jnp.where(mine, q_s[rows, :], jnp.bfloat16(0))
            logits = lax.dot_general(query, k_s[:keys, :], (((1,), (1,)), ((), ())), preferred_element_type=F32)
            logits = logits + bias_s[head, :, length - keys:]
            grown = jnp.exp(logits - jnp.max(logits, axis=1, keepdims=True))
            weights = (grown * (1.0 / jnp.sum(grown, axis=1, keepdims=True))).astype(BF16)
            context = jnp.where(mine, dot(weights, v_s[:keys, :]), context)
        ctx_s[rows, :] = context.astype(BF16)
    acc_s[...] += dot(ctx_s[...], out_w[0, 0])

    @pl.when(step == pl.num_programs(0) - 1)
    def _():
        wide = (res_ref[...].astype(F32) + acc_s[...].astype(BF16).astype(F32)).astype(BF16)
        res_ref[...] = wide
        u_ref[...] = norm_rows(wide.astype(F32), gain_out[...])


def attention(x, add, gain_in, gain_out, qkv_w, out_w, layer, rel):
    length, width = x.shape
    parts, peers, _, share, cols = qkv_w.shape
    heads = rel.shape[0] // parts
    block = rel.shape[2] - length
    head_dim = cols // heads
    rows = [x] if add is None else [x, add]
    flops = 2 * length * width * cols * 4 * parts + 4 * length * length * cols * parts * 3
    return pl.pallas_call(
        functools.partial(attention_body, heads, block, head_dim, add is not None),
        grid=(parts,),
        out_shape=[jax.ShapeDtypeStruct((length, width), BF16)] * 2,
        in_specs=[whole(length, width)] * len(rows) + [whole(1, width)] * 2 + [
            pl.BlockSpec((1, peers, 3, share, cols), lambda s: (s, 0, 0, 0, 0)),
            pl.BlockSpec((1, 1, cols, width), lambda s: (s, layer, 0, 0)),
            pl.BlockSpec((heads, 1, length + block), lambda s: (s, 0, 0))],
        out_specs=[whole(length, width)] * 2,
        scratch_shapes=[pltpu.VMEM((length, width), BF16), pltpu.VMEM((length, width), F32)]
        + [pltpu.VMEM((length, cols), BF16)] * 4 + [pltpu.VMEM((heads, block, length), F32)],
        compiler_params=params(),
        cost_estimate=cost(flops, 20e6),
        name="attention",
    )(*rows, gain_in[None], gain_out[None], qkv_w, out_w, rel)


def ffn_quarter(rows, first, second, down, acc_s):
    hidden = down.shape[0]

    def one(n, carry):
        cut = pl.ds(pl.multiple_of(n * COLS, COLS), COLS)
        act = (jax.nn.gelu(dot(rows, first[:, cut])) * dot(rows, second[:, cut])).astype(BF16)
        acc_s[...] += dot(act, down[cut, :])
        return carry

    lax.fori_loop(0, hidden // COLS, one, 0)


def expert_body(me_ref, rows_ref, *refs):
    quarters, out_ref, acc_s = refs[:-2], refs[-2], refs[-1]
    peers, slots, width = rows_ref.shape
    rows = rows_ref[...].reshape(peers * slots, width)
    acc_s[...] = jnp.zeros_like(acc_s)
    for n in range(0, len(quarters), 3):
        ffn_quarter(rows, *[ref.at[0] for ref in quarters[n:n + 3]], acc_s)
    out_ref[...] = acc_s[...].astype(BF16).reshape(out_ref.shape)


def expert(rows, which, me, own, ahead, behind, far):
    peers, slots, width = rows.shape
    count = ahead[0].shape[0]
    step = max(1, peers // 2)
    shapes = [(1, *w.shape[1:]) for w in own]
    at = [lambda s, m: (m[0] * count + which, 0, 0), lambda s, m: (which, 0, 0), lambda s, m: (which, 0, 0), lambda s, m: (0, 0, 0)]
    pieces = (own, ahead, behind, far)
    return pl.pallas_call(
        expert_body,
        grid_spec=pltpu.PrefetchScalarGridSpec(
            num_scalar_prefetch=1,
            grid=(peers // step,),
            in_specs=[pl.BlockSpec((step, slots, width), lambda s, m: (s, 0, 0))]
            + [pl.BlockSpec(shape, index) for index in at for shape in shapes],
            out_specs=pl.BlockSpec((step, slots, width), lambda s, m: (s, 0, 0)),
            scratch_shapes=[pltpu.VMEM((step * slots, width), F32)]),
        out_shape=jax.ShapeDtypeStruct((peers, slots, width), BF16),
        compiler_params=params(),
        cost_estimate=cost(24 * peers * slots * width * own[0].shape[2], 20e6),
        name="expert",
    )(me, rows, *[w for piece in pieces for w in piece])


def dense_body(u_ref, res_ref, first, second, down, out_ref, acc_s):
    acc_s[...] = jnp.zeros_like(acc_s)
    rows = u_ref[...]

    def one(q, carry):
        ffn_quarter(rows, first.at[q], second.at[q], down.at[q], acc_s)
        return carry

    lax.fori_loop(0, first.shape[0], one, 0)
    out_ref[...] = (res_ref[...].astype(F32) + acc_s[...].astype(BF16).astype(F32)).astype(BF16)


def dense(u, res, first, second, down):
    length, width = u.shape
    step = length // 2
    block = pl.BlockSpec((step, width), lambda s: (s, 0))
    return pl.pallas_call(
        dense_body,
        grid=(length // step,),
        out_shape=jax.ShapeDtypeStruct((length, width), BF16),
        in_specs=[block, block, whole(*first.shape), whole(*second.shape), whole(*down.shape)],
        out_specs=block,
        scratch_shapes=[pltpu.VMEM((step, width), F32)],
        compiler_params=params(),
        cost_estimate=cost(6 * length * first.size, 18e6),
        name="dense",
    )(u, res, first, second, down)


def positions(idx_first, idx_second, experts):
    tokens = idx_first.shape[0]
    block = min(256, tokens)
    lane = jnp.arange(2 * experts, dtype=jnp.int32)
    hot = (idx_first[:, None] == lane) | (idx_second[:, None] + experts == lane)
    cells = hot.astype(BF16).reshape(tokens // block, block, 2 * experts)
    lower = jnp.tril(jnp.ones((block, block), BF16))
    within = jnp.einsum("ij,bjn->bin", lower, cells, preferred_element_type=F32)
    totals = within[:, -1, :]
    before = jnp.cumsum(totals, axis=0) - totals
    count = jnp.sum(totals, axis=0)
    shift = jnp.concatenate([jnp.zeros((experts,), F32), count[:experts]]) - 1.0
    ranks = (within + (before + shift)[:, None, :]).reshape(tokens, 2 * experts)
    ranks = jnp.where(hot, ranks, 0.0)
    first = jnp.sum(jnp.where(lane < experts, ranks, 0.0), axis=1)
    second = jnp.sum(jnp.where(lane < experts, 0.0, ranks), axis=1)
    return first.astype(jnp.int32), second.astype(jnp.int32)


def tokens_of_slots(choice, place, owned, capacity):
    number = jnp.arange(1, choice.shape[1] + 1, dtype=jnp.int32)
    number = jnp.concatenate([number, number])
    mine = choice.reshape(-1)[None, :] == owned[:, None]
    high = jnp.where(mine, number // 128, 0).astype(BF16)
    low = jnp.where(mine, number % 128, 0).astype(BF16)
    at_slot = (place.reshape(-1)[:, None] == jnp.arange(capacity, dtype=jnp.int32)).astype(BF16)
    found = dot(jnp.concatenate([high, low]), at_slot).astype(jnp.int32)
    return jnp.maximum(found[: owned.shape[0]] * 128 + found[owned.shape[0]:] - 1, 0)


def pick_body(half, token, *refs):
    chunks, (out0, out1, wide_s, stage_s) = refs[:-4], refs[-4:]
    step = pl.program_id(0)
    block = stage_s.shape[0]

    @pl.when(step == 0)
    def _():
        for n, ref in enumerate(chunks):
            wide_s[n * ref.shape[0]:(n + 1) * ref.shape[0]] = ref[...].astype(F32)

    def eight(n, carry):
        for k in range(8):
            at = n * 8 + k
            stage_s[pl.ds(at, 1), :] = wide_s[pl.ds(token[step * block + at], 1), :]
        return carry

    lax.fori_loop(0, block // 8, eight, 0)

    @pl.when(step < half)
    def _():
        out0[...] = stage_s[...].astype(BF16)

    @pl.when(step >= half)
    def _():
        out1[...] = stage_s[...].astype(BF16)


def pick(chunks, token):
    count = token.shape[0]
    width = chunks[0].shape[1]
    block = min(512, count // 2)
    half = count // 2 // block
    return pl.pallas_call(
        functools.partial(pick_body, half),
        grid=(2 * half,),
        out_shape=[jax.ShapeDtypeStruct((count // 2, width), BF16)] * 2,
        in_specs=[pl.BlockSpec(memory_space=pltpu.SMEM)] + [whole(*c.shape) for c in chunks],
        out_specs=[pl.BlockSpec((block, width), lambda s: (jnp.minimum(s, half - 1), 0)),
                   pl.BlockSpec((block, width), lambda s: (jnp.maximum(s - half, 0), 0))],
        scratch_shapes=[pltpu.VMEM((len(chunks) * chunks[0].shape[0], width), F32), pltpu.VMEM((block, width), F32)],
        compiler_params=params(),
        cost_estimate=cost(20e9, 20e6),
        name="pick",
    )(token, *chunks)


def join_body(half, a_ref, b_ref, out_ref):
    step = pl.program_id(0)

    @pl.when(step < half)
    def _():
        out_ref[...] = a_ref[...]

    @pl.when(step >= half)
    def _():
        out_ref[...] = b_ref[...]


def join(a, b):
    rows, width = a.shape
    block = min(1024, rows)
    half = rows // block
    return pl.pallas_call(
        functools.partial(join_body, half),
        grid=(2 * half,),
        out_shape=jax.ShapeDtypeStruct((2 * rows, width), BF16),
        in_specs=[pl.BlockSpec((block, width), lambda s: (jnp.minimum(s, half - 1), 0)),
                  pl.BlockSpec((block, width), lambda s: (jnp.maximum(s - half, 0), 0))],
        out_specs=pl.BlockSpec((block, width), lambda s: (s, 0)),
        compiler_params=params(),
        cost_estimate=cost(5e9, 25e6),
        name="join",
    )(a, b)


def combine_body(r1, r2, g1, g2, y0, y1, out_ref, wide_s, stage_s):
    step = pl.program_id(0)
    rows = y0.shape[0]
    block = out_ref.shape[0]

    @pl.when(step == 0)
    def _():
        wide_s[:rows] = y0[...].astype(F32)
        wide_s[rows:2 * rows] = y1[...].astype(F32)
        wide_s[2 * rows:] = jnp.zeros_like(wide_s[2 * rows:])

    def eight(n, carry):
        for k in range(8):
            at = n * 8 + k
            t = step * block + at
            stage_s[pl.ds(at, 1), :] = g1[t] * wide_s[pl.ds(r1[t], 1), :] + g2[t] * wide_s[pl.ds(r2[t], 1), :]
        return carry

    lax.fori_loop(0, block // 8, eight, 0)
    out_ref[...] = stage_s[...].astype(BF16)


def combine(rows, gates, y0, y1):
    tokens = rows[0].shape[0]
    width = y0.shape[1]
    block = min(512, tokens)
    smem = pl.BlockSpec(memory_space=pltpu.SMEM)
    return pl.pallas_call(
        combine_body,
        grid=(tokens // block,),
        out_shape=jax.ShapeDtypeStruct((tokens, width), BF16),
        in_specs=[smem] * 4 + [whole(*y0.shape)] * 2,
        out_specs=pl.BlockSpec((block, width), lambda s: (s, 0)),
        scratch_shapes=[pltpu.VMEM((2 * y0.shape[0] + 8, width), F32), pltpu.VMEM((block, width), F32)],
        compiler_params=params(),
        cost_estimate=cost(20e9, 20e6),
        name="combine",
    )(*rows, *gates, y0, y1)


def solution(mesh):
    row_spec = P(("part", "ep"))
    in_specs = (row_spec, row_spec, row_spec, P(None, "tp"), P(), P(None, None, None, "tp"), P(None, "tp"), P(), P("ep", None, "tp"), P("ep", None, "tp"), P("ep", "tp"), P(None, "tp"), P(None, "tp"), P("tp"))
    tp, ep = mesh.shape["tp"], mesh.shape["ep"]
    up = [(d, (d + 1) % tp) for d in range(tp)]
    back = [(d, (d - 1) % tp) for d in range(tp)]

    def device_step(x_in, idx_first, idx_second, rel_bias, norm_gain, attn_qkv, attn_out, gate_w, expert_w0, expert_w1, expert_down, dense_w0, dense_w1, dense_down):
        num_seqs, length, width = x_in.shape
        experts = gate_w.shape[1]
        tokens = num_seqs * length
        capacity = (2 * tokens + experts - 1) // experts
        me, spot = lax.axis_index("tp"), lax.axis_index("ep")
        chunks = num_seqs // tp
        layers = attn_qkv.shape[0]
        held = experts // ep
        count = held // tp
        block = min(256, length)

        def gather_all(piece):
            return lax.all_gather(piece, ("tp", "ep"), axis=0, tiled=False)

        def gather_rows(weight):
            rows = weight.shape[0] // ep
            return lax.dynamic_slice_in_dim(weight, spot * rows, rows, 0)

        share = width // ep
        cols = attn_qkv.shape[3]
        split = ep // layers
        out_piece = lax.dynamic_slice(attn_out, (spot // split, spot % split * (cols // split), 0), (1, cols // split, width))[0]
        qkv_piece = [lax.dynamic_slice(attn_qkv, (n, 0, spot * share, 0), (1, 3, share, cols))[0] for n in range(layers)]
        dense_piece = [gather_rows(w) for w in (dense_w0, dense_w1, dense_down)]
        out_w = gather_all(out_piece).reshape(tp, layers, cols, width)
        qkv_0 = gather_all(qkv_piece[0]).reshape(tp, ep, 3, share, cols)
        rel = lax.all_gather(rel_bias, "tp", axis=1, tiled=True)[:, :, None, ::-1]
        rel = jnp.concatenate([rel, jnp.full((*rel.shape[:3], block), MASKED, F32)], axis=3)

        expert_w = (expert_w0, expert_w1, expert_down)

        def pieces(owner):
            return [lax.dynamic_slice_in_dim(w, owner * count, count, 0) for w in expert_w]

        near = [pieces((me + 1) % tp), pieces((me - 1) % tp)]
        far = [[w[n:n + 1] for w in pieces((me + 2) % tp)] for n in range(count)]
        late = (qkv_piece[1], dense_piece)
        near, far, rel = lax.optimization_barrier((near, far, rel))

        far = [[lax.ppermute(w, "tp", (up, back)[n % 2]) for w in far[n]] for n in range(count)]
        from_behind = [lax.ppermute(w, "tp", up) for w in near[0]]
        from_ahead = [lax.ppermute(w, "tp", back) for w in near[1]]
        qkv_1 = gather_all(late[0]).reshape(tp, ep, 3, share, cols)
        dense_w = [gather_all(w).reshape(tp, *full.shape) for w, full in zip(late[1], (dense_w0, dense_w1, dense_down))]

        res, sent = [], []
        for c in range(chunks):
            x = lax.dynamic_index_in_dim(x_in, c * tp + me, 0, keepdims=False)
            r, u = attention(x, None, norm_gain[0], norm_gain[1], qkv_0, out_w, 0, rel[0])
            res.append(r)
            sent.append(lax.all_gather(u, "tp", axis=0, tiled=True))
        sent, far = lax.optimization_barrier((sent, far))
        far = [[lax.ppermute(w, "tp", (up, back)[n % 2]) for w in far[n]] for n in range(count)]

        first_idx, second_idx, _ = lax.optimization_barrier((idx_first.reshape(-1), idx_second.reshape(-1), u))
        place = positions(first_idx, second_idx, experts)
        owned = (jnp.arange(count, dtype=jnp.int32)[:, None] + me * count + jnp.arange(ep, dtype=jnp.int32) * held).reshape(-1)
        slot_token = tokens_of_slots(jnp.stack([first_idx, second_idx]), jnp.stack(place), owned, capacity).reshape(-1)

        send = pick(sent, slot_token)
        recv = [lax.all_to_all(send[e].reshape(ep, capacity, width), "ep", 0, 0, tiled=True) for e in range(count)]
        recv[0], qkv_1, dense_w = lax.optimization_barrier((recv[0], qkv_1, dense_w))

        lane = jnp.arange(experts, dtype=jnp.int32)
        probs = [jax.nn.softmax(jnp.dot(u, gate_w, preferred_element_type=F32), axis=-1) for u in sent]
        none = count * ep * capacity
        span = tp * length
        rows, gates = [[], []], []
        for c in range(chunks):
            cut = slice(c * span, (c + 1) * span)
            both = [jnp.sum(jnp.where(idx[cut, None] == lane, probs[c], 0.0), axis=1) for idx in (first_idx, second_idx)]
            total = both[0] + both[1]
            gates.append([g / total for g in both])
            for n, idx in enumerate((first_idx[cut], second_idx[cut])):
                local = idx % held
                slot = place[n][cut]
                mine = (slot < capacity) & (local // count == me)
                rows[c].append(jnp.where(mine, (local % count) * (ep * capacity) + idx // held * capacity + slot, none))

        me_ref = me.astype(jnp.int32)[None]
        returned = []
        for e in range(count):
            y = expert(recv[e], e, me_ref, expert_w, from_behind, from_ahead, far[e])
            returned.append(lax.all_to_all(y, "ep", 0, 0, tiled=True).reshape(ep * capacity, width))

        outs = []
        for c in range(chunks):
            part = combine(rows[c], gates[c], *returned)
            mixed = lax.psum_scatter(part, "tp", scatter_dimension=0, tiled=True)
            r, u = attention(res[c], mixed, norm_gain[2], norm_gain[3], qkv_1, out_w, 1, rel[1])
            out = dense(u, r, *dense_w)
            outs.append(lax.all_gather(out, "tp", axis=0, tiled=True))
        return join(*outs).reshape(num_seqs, length, width)

    return jax.shard_map(device_step, mesh=mesh, in_specs=in_specs, out_specs=row_spec, check_vma=False)
```

```python
import functools

import jax
import jax.numpy as jnp
from jax import lax
from jax.experimental import pallas as pl
from jax.experimental.pallas import tpu as pltpu
from jax.sharding import PartitionSpec as P


F32 = jnp.float32
BF16 = jnp.bfloat16
MASKED = -1e30
VMEM_BYTES = 60 << 20
COLS = 256
LANES = 128
TILE = 8


def dot(a, b):
    return jnp.dot(a, b, preferred_element_type=F32)


def norm_rows(wide, gain):
    scale = lax.rsqrt(jnp.mean(wide * wide, axis=-1, keepdims=True) + 1e-6)
    return (wide * scale * gain).astype(BF16)


def whole(*shape):
    return pl.BlockSpec(shape, lambda *_: (0,) * len(shape))


def params():
    return pltpu.CompilerParams(vmem_limit_bytes=VMEM_BYTES)


def cost(flops, nbytes):
    return pl.CostEstimate(flops=int(flops), bytes_accessed=int(nbytes), transcendentals=0)


def attention_body(heads, block, head_dim, layer, has_add, *refs):
    x_ref, refs = refs[0], refs[1:]
    if has_add:
        add_ref, refs = refs[0], refs[1:]
    gain_in, gain_out, qkv_w, out_w, rel_ref, res_ref, u_ref, src_s, acc_s, q_s, k_s, v_s, ctx_s, bias_s = refs
    step = pl.program_id(0)
    length, width = x_ref.shape
    cols = q_s.shape[1]

    @pl.when(step == 0)
    def _():
        wide = x_ref[...].astype(F32)
        if has_add:
            wide = (wide + add_ref[...].astype(F32)).astype(BF16).astype(F32)
        res_ref[...] = wide.astype(BF16)
        src_s[...] = norm_rows(wide, gain_in[...])
        acc_s[...] = jnp.zeros_like(acc_s)

    weight = qkv_w[:, 0].reshape(width, width)
    q_s[...] = dot(src_s[...], weight[:, :cols]).astype(BF16) * jnp.bfloat16(head_dim ** -0.5)
    k_s[...] = dot(src_s[...], weight[:, cols:2 * cols]).astype(BF16)
    v_s[...] = dot(src_s[...], weight[:, 2 * cols:3 * cols]).astype(BF16)
    lane = lax.broadcasted_iota(jnp.int32, (block, cols), 1)
    span = length + block
    terms = rel_ref[:, 0].astype(F32)
    reach = length // terms.shape[0]
    rows = [terms[e, 0:1] + terms[e, 1:2] + terms[e, 2:3] for e in range(terms.shape[0])]
    for head in range(heads):
        at = (layer * heads + head) * reach
        table = jnp.concatenate([row[:, at:at + reach] for row in rows] + [jnp.full((1, block), MASKED, F32)], axis=1)
        spread = jnp.broadcast_to(table, (block, span))
        bias_s[head] = pltpu.roll(spread, span - block + 1, 1, stride=1, stride_axis=0)[:, :length]
    items = [(part, head) for part in range(length // block) for head in range(heads)]

    def scores(part, head):
        keys = (part + 1) * block
        mine = (lane >= head * head_dim) & (lane < (head + 1) * head_dim)
        query = jnp.where(mine, q_s[pl.ds(part * block, block), :], jnp.bfloat16(0))
        logits = lax.dot_general(query, k_s[:keys, :], (((1,), (1,)), ((), ())), preferred_element_type=F32)
        return logits + bias_s[head, :, length - keys:]

    ahead = scores(*items[0])
    context = None
    for n, (part, head) in enumerate(items):
        keys = (part + 1) * block
        logits = ahead
        if n + 1 < len(items):
            ahead = scores(*items[n + 1])
        mine = (lane >= head * head_dim) & (lane < (head + 1) * head_dim)
        grown = jnp.exp(logits - jnp.max(logits, axis=1, keepdims=True))
        weights = (grown * (1.0 / jnp.sum(grown, axis=1, keepdims=True))).astype(BF16)
        out = dot(weights, v_s[:keys, :])
        context = out if head == 0 else jnp.where(mine, out, context)
        if head == heads - 1:
            ctx_s[pl.ds(part * block, block), :] = context.astype(BF16)
    acc_s[...] += dot(ctx_s[:, :heads * head_dim], out_w[:, 0].reshape(heads * head_dim, width))

    @pl.when(step == pl.num_programs(0) - 1)
    def _():
        wide = (res_ref[...].astype(F32) + acc_s[...].astype(BF16).astype(F32)).astype(BF16)
        res_ref[...] = wide
        u_ref[...] = norm_rows(wide.astype(F32), gain_out[...])


def attention(x, add, gain_in, gain_out, layer_w, out_at, first_w, layer, heads, block):
    length, width = x.shape
    peers, parts, first_rows, _ = first_w.shape
    share = width // peers
    head_dim = width // (parts * heads)
    span = heads * head_dim
    cols = -(-span // LANES) * LANES
    out_rows = span // peers
    inputs = [x] if add is None else [x, add]
    flops = 2 * length * width * cols * 4 * parts + 4 * length * length * cols * parts * 3
    return pl.pallas_call(
        functools.partial(attention_body, heads, block, head_dim, layer, add is not None),
        grid=(parts,),
        out_shape=[jax.ShapeDtypeStruct((length, width), BF16)] * 2,
        in_specs=[whole(length, width)] * len(inputs) + [whole(1, width)] * 2 + [
            pl.BlockSpec((peers, 1, share, width), lambda s: (0, s, 0, 0)),
            pl.BlockSpec((peers, 1, out_rows, width), lambda s: (0, s, out_at // out_rows, 0)),
            pl.BlockSpec((peers, 1, TILE, width), lambda s: (0, s, first_rows // TILE - 1, 0))],
        out_specs=[whole(length, width)] * 2,
        scratch_shapes=[pltpu.VMEM((length, width), BF16), pltpu.VMEM((length, width), F32)]
        + [pltpu.VMEM((length, cols), BF16)] * 4 + [pltpu.VMEM((heads, block, length), F32)],
        compiler_params=params(),
        cost_estimate=cost(flops, 20e6),
        name="attention",
    )(*inputs, gain_in[None], gain_out[None], layer_w, layer_w, first_w)


def ffn_quarter(rows, first, second, down, hidden, acc_s, fresh):
    @pl.when(fresh)
    def _():
        acc_s[...] = jnp.zeros_like(acc_s)

    def one(n, carry):
        cut = pl.ds(pl.multiple_of(n * COLS, COLS), COLS)
        act = (jax.nn.gelu(dot(rows, first(cut))) * dot(rows, second(cut))).astype(BF16)
        acc_s[...] += dot(act, down(cut))
        return carry

    lax.fori_loop(0, hidden // COLS, one, 0)


def ffn_body(plan, has_acc, last, me_ref, rows_ref, *refs):
    sources, refs = refs[:len(plan)], refs[len(plan):]
    if has_acc:
        acc_in, refs = refs[0], refs[1:]
    out_ref, weight_s, sems, acc_s = refs
    step = pl.program_id(0)
    rows = rows_ref[...].reshape(-1, rows_ref.shape[-1])
    quarters = weight_s.shape[0]

    def copy(n):
        quarter, matrix, rows, cols, mine = plan[n]
        which = me_ref[0] if mine else 0
        return pltpu.make_async_copy(sources[n].at[which], weight_s.at[quarter, matrix, pl.ds(*rows), pl.ds(*cols)], sems.at[n])

    @pl.when(step == 0)
    def _():
        for n in range(len(plan)):
            copy(n).start()

    if has_acc:
        acc_s[...] = acc_in[...].reshape(acc_s.shape)

    def one(q, carry):
        for n in range(len(plan)):
            @pl.when((step == 0) & (q == plan[n][0]))
            def _():
                copy(n).wait()

        ffn_quarter(rows, lambda cut: weight_s[q, 0, :, cut], lambda cut: weight_s[q, 1, :, cut], lambda cut: weight_s[q, 2, cut, :],
                    weight_s.shape[3], acc_s, (q == 0) & (not has_acc))
        return carry

    lax.fori_loop(0, quarters, one, 0)
    out_ref[...] = (acc_s[...].astype(BF16) if last else acc_s[...]).reshape(out_ref.shape)


def expert(rows, quarters, index, acc, last):
    peers, slots, width = rows.shape
    step = max(1, peers // 2)
    hidden = sum(array.shape[1] for array, _ in quarters[0][2])
    plan, sources = [], []
    for q, quarter in enumerate(quarters):
        for matrix, pieces in enumerate(quarter):
            at, col = 0, 0
            limit = width if matrix == 2 else hidden
            for array, mine in pieces:
                plan.append((q, matrix, (at, array.shape[1]), (col, array.shape[2]), mine))
                sources.append(array)
                col += array.shape[2]
                if col == limit:
                    at, col = at + array.shape[1], 0
    block = pl.BlockSpec((step, slots, width), lambda s, m: (s, 0, 0))
    return pl.pallas_call(
        functools.partial(ffn_body, plan, acc is not None, last),
        grid_spec=pltpu.PrefetchScalarGridSpec(
            num_scalar_prefetch=1,
            grid=(peers // step,),
            in_specs=[block] + [pl.BlockSpec(memory_space=pl.ANY)] * len(sources) + [block] * (acc is not None),
            out_specs=block,
            scratch_shapes=[pltpu.VMEM((len(quarters), 3, width, hidden), BF16), pltpu.SemaphoreType.DMA((len(plan),)),
                            pltpu.VMEM((step * slots, width), F32)]),
        out_shape=jax.ShapeDtypeStruct((peers, slots, width), BF16 if last else F32),
        compiler_params=params(),
        cost_estimate=cost(6 * peers * slots * width * hidden * len(quarters), 20e6),
        name="expert",
    )(index, rows, *sources, *([] if acc is None else [acc]))


def dense_body(u_ref, res_ref, late_ref, out_ref, weight_s, sems, acc_s):
    peers, parts, _, _ = late_ref.shape
    hidden = weight_s.shape[2]
    share = hidden // peers
    rows = u_ref[...]

    def copy(q, matrix, peer):
        return pltpu.make_async_copy(late_ref.at[peer, q, pl.ds((1 + matrix) * share, share)],
                                     weight_s.at[q, matrix, pl.ds(peer * share, share)], sems.at[q])

    def start(q, carry):
        for matrix in range(3):
            for peer in range(peers):
                copy(q, matrix, peer).start()
        return carry

    def one(q, carry):
        for matrix in range(3):
            for peer in range(peers):
                copy(q, matrix, peer).wait()
        ffn_quarter(rows, lambda cut: weight_s[q, 0, :, cut], lambda cut: weight_s[q, 1, :, cut], lambda cut: weight_s[q, 2, cut, :],
                    hidden, acc_s, q == 0)
        return carry

    lax.fori_loop(0, parts, start, 0)
    lax.fori_loop(0, parts, one, 0)
    out_ref[...] = (res_ref[...].astype(F32) + acc_s[...].astype(BF16).astype(F32)).astype(BF16)


def dense(u, res, late_w):
    length, width = u.shape
    peers, parts = late_w.shape[:2]
    share = width // peers
    return pl.pallas_call(
        dense_body,
        out_shape=jax.ShapeDtypeStruct((length, width), BF16),
        in_specs=[pl.BlockSpec(memory_space=pltpu.VMEM)] * 2 + [pl.BlockSpec(memory_space=pl.ANY)],
        out_specs=pl.BlockSpec(memory_space=pltpu.VMEM),
        scratch_shapes=[pltpu.VMEM((parts, 3, peers * share, width), BF16), pltpu.SemaphoreType.DMA((parts,)),
                        pltpu.VMEM((length, width), F32)],
        compiler_params=params(),
        cost_estimate=cost(6 * length * width * width * parts, 18e6),
        name="dense",
    )(u, res, late_w)


def positions(idx_first, idx_second, experts):
    tokens = idx_first.shape[0]
    block = min(256, tokens)
    lane = jnp.arange(2 * experts, dtype=jnp.int32)
    hot = (idx_first[:, None] == lane) | (idx_second[:, None] + experts == lane)
    cells = hot.astype(BF16).reshape(tokens // block, block, 2 * experts)
    lower = jnp.tril(jnp.ones((block, block), BF16))
    within = jnp.einsum("ij,bjn->bin", lower, cells, preferred_element_type=F32)
    totals = within[:, -1, :]
    before = jnp.cumsum(totals, axis=0) - totals
    count = jnp.sum(totals, axis=0)
    shift = jnp.concatenate([jnp.zeros((experts,), F32), count[:experts]]) - 1.0
    ranks = (within + (before + shift)[:, None, :]).reshape(tokens, 2 * experts)
    ranks = jnp.where(hot, ranks, 0.0)
    first = jnp.sum(jnp.where(lane < experts, ranks, 0.0), axis=1)
    second = jnp.sum(jnp.where(lane < experts, 0.0, ranks), axis=1)
    return first.astype(jnp.int32), second.astype(jnp.int32)


def tokens_of_slots(choice, place, owned, capacity):
    number = jnp.arange(1, choice.shape[1] + 1, dtype=jnp.int32)
    number = jnp.concatenate([number, number])
    mine = choice.reshape(-1)[None, :] == owned[:, None]
    high = jnp.where(mine, number // 128, 0).astype(BF16)
    low = jnp.where(mine, number % 128, 0).astype(BF16)
    at_slot = (place.reshape(-1)[:, None] == jnp.arange(capacity, dtype=jnp.int32)).astype(BF16)
    found = dot(jnp.concatenate([high, low]), at_slot).astype(jnp.int32)
    return jnp.maximum(found[: owned.shape[0]] * 128 + found[owned.shape[0]:] - 1, 0)


def to_tiles(tiles, base, ref):
    rows, width = ref.shape

    def sixteen(n, carry):
        r = pl.multiple_of(n * 16, 16)
        for k in range(width // LANES):
            values = ref[pl.ds(r, 16), k * LANES:(k + 1) * LANES].astype(F32)
            for h in range(2):
                tiles[pl.ds((base + r + h * TILE) * TILE + k, TILE, stride=TILE), :] = values[h * TILE:(h + 1) * TILE]
        return carry

    lax.fori_loop(0, rows // 16, sixteen, 0)


def from_tiles(tiles, ref):
    rows, width = ref.shape

    def sixteen(n, carry):
        r = pl.multiple_of(n * 16, 16)
        for k in range(width // LANES):
            values = [tiles[pl.ds((r + h * TILE) * TILE + k, TILE, stride=TILE), :] for h in range(2)]
            ref[pl.ds(r, 16), k * LANES:(k + 1) * LANES] = jnp.concatenate(values).astype(BF16)
        return carry

    lax.fori_loop(0, rows // 16, sixteen, 0)


def tile_at(index):
    return pl.ds(pl.multiple_of(index, TILE), TILE)


def pick_body(half, at_ref, *refs):
    pieces, (out0, out1, tiles, stage) = refs[:-4], refs[-4:]
    step = pl.program_id(0)
    block = out0.shape[0]

    @pl.when(step == 0)
    def _():
        base = 0
        for ref in pieces:
            to_tiles(tiles, base, ref)
            base += ref.shape[0]

    def eight(n, carry):
        for k in range(TILE):
            row = n * TILE + k
            stage[tile_at(row * TILE), :] = tiles[tile_at(at_ref[step * block + row]), :]
        return carry

    lax.fori_loop(0, block // TILE, eight, 0)

    @pl.when(step < half)
    def _():
        from_tiles(stage, out0)

    @pl.when(step >= half)
    def _():
        from_tiles(stage, out1)


def pick(pieces, at):
    count = at.shape[0]
    width = pieces[0].shape[1]
    rows = sum(p.shape[0] for p in pieces)
    block = min(512, count // 2)
    half = count // 2 // block
    return pl.pallas_call(
        functools.partial(pick_body, half),
        grid=(2 * half,),
        out_shape=[jax.ShapeDtypeStruct((count // 2, width), BF16)] * 2,
        in_specs=[pl.BlockSpec(memory_space=pltpu.SMEM)] + [pl.BlockSpec(p.shape, lambda s: (0, 0), pipeline_mode=pl.Buffered(1)) for p in pieces],
        out_specs=[pl.BlockSpec((block, width), lambda s: (jnp.minimum(s, half - 1), 0)),
                   pl.BlockSpec((block, width), lambda s: (jnp.maximum(s - half, 0), 0))],
        scratch_shapes=[pltpu.VMEM((rows * TILE, LANES), F32), pltpu.VMEM((block * TILE, LANES), F32)],
        compiler_params=pltpu.CompilerParams(vmem_limit_bytes=62 << 20),
        cost_estimate=cost(20e9, 20e6),
        name="pick",
    )(at, *pieces)


def combine_body(r1, r2, g1, g2, y0, y1, out_ref, tiles, stage):
    step = pl.program_id(0)
    rows, _ = y0.shape
    block = out_ref.shape[0]

    @pl.when(step == 0)
    def _():
        to_tiles(tiles, 0, y0)
        to_tiles(tiles, rows, y1)
        tiles[pl.ds(2 * rows * TILE, TILE), :] = jnp.zeros((TILE, LANES), F32)

    def eight(n, carry):
        for k in range(TILE):
            row = n * TILE + k
            t = step * block + row
            stage[tile_at(row * TILE), :] = g1[t] * tiles[tile_at(r1[t]), :] + g2[t] * tiles[tile_at(r2[t]), :]
        return carry

    lax.fori_loop(0, block // TILE, eight, 0)
    from_tiles(stage, out_ref)


def combine(rows, gates, y0, y1):
    tokens = rows[0].shape[0]
    width = y0.shape[1]
    block = min(512, tokens)
    smem = pl.BlockSpec(memory_space=pltpu.SMEM)
    return pl.pallas_call(
        combine_body,
        grid=(tokens // block,),
        out_shape=jax.ShapeDtypeStruct((tokens, width), BF16),
        in_specs=[smem] * 4 + [whole(*y0.shape)] * 2,
        out_specs=pl.BlockSpec((block, width), lambda s: (s, 0)),
        scratch_shapes=[pltpu.VMEM(((2 * y0.shape[0] + 1) * TILE, LANES), F32), pltpu.VMEM((block * TILE, LANES), F32)],
        compiler_params=params(),
        cost_estimate=cost(15e9, 20e6),
        name="combine",
    )(*rows, *gates, y0, y1)


def place_body(plan, row_ref, *refs):
    pieces, out_ref, sems = refs[:len(plan)], refs[-2], refs[-1]
    copies = []
    for n, (turn, at) in enumerate(plan):
        row = pl.multiple_of(row_ref[turn] + at, 2 * TILE)
        copies.append(pltpu.make_async_copy(pieces[n], out_ref.at[pl.ds(row, pieces[n].shape[0])], sems.at[n]))
    for copy in copies:
        copy.start()
    for copy in copies:
        copy.wait()


def place(plan, rows, pieces, out):
    fresh = isinstance(out, tuple)
    return pl.pallas_call(
        functools.partial(place_body, plan),
        out_shape=jax.ShapeDtypeStruct(out if fresh else out.shape, BF16),
        in_specs=[pl.BlockSpec(memory_space=pltpu.SMEM)] + [pl.BlockSpec(memory_space=pltpu.VMEM)] * len(pieces)
        + [pl.BlockSpec(memory_space=pl.ANY)] * (not fresh),
        out_specs=pl.BlockSpec(memory_space=pl.ANY),
        scratch_shapes=[pltpu.SemaphoreType.DMA((len(pieces),))],
        input_output_aliases={} if fresh else {1 + len(pieces): 0},
        compiler_params=params(),
        cost_estimate=cost(3e9, 12e6),
        name="place",
    )(rows, *pieces, *([] if fresh else [out]))


def split_terms(wide):
    terms = []
    for _ in range(3):
        term = lax.reduce_precision(wide, exponent_bits=8, mantissa_bits=7)
        terms.append(term.astype(BF16))
        wide = wide - term
    return terms


def pack_qkv(weight, layer, spot, share, cols):
    piece = lax.dynamic_slice(weight, (layer, 0, spot * share, 0), (1, 3, share, weight.shape[3]))[0]
    piece = jnp.pad(piece, ((0, 0), (0, 0), (0, cols - piece.shape[2])))
    return jnp.concatenate([piece[n] for n in range(3)], axis=1)


def pack_out(attn_out, layer, spot, ep):
    rows = attn_out.shape[1] // ep
    return lax.dynamic_slice(attn_out, (layer, spot * rows, 0), (1, rows, attn_out.shape[2]))[0]


def pack_rel(rel_bias, width, spot, ep):
    length = rel_bias.shape[2]
    reach = length // ep
    backward = rel_bias.reshape(-1, length)[:, ::-1]
    terms = split_terms(lax.dynamic_slice_in_dim(backward, spot * reach, reach, 1).reshape(1, width))
    return jnp.concatenate(terms + [jnp.zeros((TILE - 3, width), BF16)])


def solution(mesh):
    row_spec = P(("part", "ep"))
    in_specs = (row_spec, row_spec, row_spec, P(None, "tp"), P(), P(None, None, None, "tp"), P(None, "tp"), P(), P("ep", None, "tp"), P("ep", None, "tp"), P("ep", "tp"), P(None, "tp"), P(None, "tp"), P("tp"))
    tp, ep = mesh.shape["tp"], mesh.shape["ep"]
    up = [(d, (d + 1) % tp) for d in range(tp)]
    back = [(d, (d - 1) % tp) for d in range(tp)]

    def device_step(x_in, idx_first, idx_second, rel_bias, norm_gain, attn_qkv, attn_out, gate_w, expert_w0, expert_w1, expert_down, dense_w0, dense_w1, dense_down):
        num_seqs, length, width = x_in.shape
        experts = gate_w.shape[1]
        tokens = num_seqs * length
        capacity = (2 * tokens + experts - 1) // experts
        me, spot = lax.axis_index("tp"), lax.axis_index("ep")
        chunks = num_seqs // tp
        held = experts // ep
        count = held // tp
        block = min(256, length)
        share = width // ep
        heads = rel_bias.shape[1]
        cols = -(-attn_qkv.shape[3] // LANES) * LANES

        def send_up(w):
            return lax.ppermute(w, "tp", up)

        def send_back(w):
            return lax.ppermute(w, "tp", back)

        def over_tp(piece):
            return lax.all_gather(piece, "tp", axis=0, tiled=False)

        def over_ep(piece):
            return lax.all_gather(piece, "ep", axis=0, tiled=False)

        first = jnp.concatenate([pack_qkv(attn_qkv, 0, spot, share, cols), pack_out(attn_out, 0, spot, ep), pack_rel(rel_bias, width, spot, ep)])
        first_w = over_ep(over_tp(first))
        late = jnp.concatenate([pack_qkv(attn_qkv, 1, spot, share, cols)]
                               + [lax.dynamic_slice_in_dim(w, spot * share, share, 0) for w in (dense_w0, dense_w1, dense_down)]
                               + [pack_out(attn_out, 1, spot, ep)])

        weights = (expert_w0, expert_w1, expert_down)

        def quarter(owner, e):
            return [lax.dynamic_slice_in_dim(w, owner * count + e, 1, 0) for w in weights]

        half = expert_down.shape[1] // 2
        far_up, far_back = [], []
        for e in range(count):
            w0, w1, wd = quarter((me + 2) % tp, e)
            far_up.append([w0, wd[:, :half]])
            far_back.append([w1, wd[:, half:]])

        def halves(w0, w1, wd):
            return [[w0[:, :, cut], w1[:, :, cut], wd[:, cut]] for cut in (slice(0, half), slice(half, 2 * half))]

        near_up = [[quarter((me + 1) % tp, e)] for e in range(count - 1)] + [halves(*quarter((me + 1) % tp, count - 1))]
        near_back = [[quarter((me - 1) % tp, e)] for e in range(count - 1)] + [halves(*quarter((me - 1) % tp, count - 1))]

        x = [lax.dynamic_index_in_dim(x_in, c * tp + me, 0, keepdims=False) for c in range(chunks)]
        far_back[-1][-1], near_up, near_back, x = lax.optimization_barrier((far_back[-1][-1], near_up, near_back, x))

        far_up = [[send_up(w) for w in ws] for ws in far_up]
        far_back = [[send_back(w) for w in ws] for ws in far_back]
        late = over_tp(late)
        late_w = over_ep(late)
        res, own, behind, ahead, across = [], [], [], [], []
        for c in range(chunks):
            r, u = attention(x[c], None, norm_gain[0], norm_gain[1], first_w, share, first_w, 0, heads, block)
            res.append(r)
            own.append(u)
            behind.append(send_up(u))
            ahead.append(send_back(u))

        first_idx, second_idx, _ = lax.optimization_barrier((idx_first.reshape(-1), idx_second.reshape(-1), own[-1]))
        ranks = positions(first_idx, second_idx, experts)
        owned = (jnp.arange(count, dtype=jnp.int32)[:, None] + me * count + jnp.arange(ep, dtype=jnp.int32) * held).reshape(-1)
        token = tokens_of_slots(jnp.stack([first_idx, second_idx]), jnp.stack(ranks), owned, capacity).reshape(-1)
        seq = token // length
        turn = (seq % tp - me) % tp
        turn = jnp.where(turn == tp - 1, 1, jnp.where(turn == 1, 2, jnp.where(turn == 2, 3, 0)))
        at = (((seq // tp) * tp + turn) * length + token % length) * TILE

        mid = length // 2
        for c in range(chunks):
            if c == chunks - 1:
                behind[c], ahead[c], near_up, near_back, at = lax.optimization_barrier((behind[c], ahead[c], near_up, near_back, at))
            across.append([send_up(behind[c][:mid]), send_back(ahead[c][mid:])])
        from_behind, from_ahead, far = [], [], []
        for e in range(count):
            from_behind.append([[send_up(w) for w in ws] for ws in near_up[e]])
            from_ahead.append([[send_back(w) for w in ws] for ws in near_back[e]])
            far.append(([send_up(w) for w in far_up[e]], [send_back(w) for w in far_back[e]]))

        pieces = [p for c in range(chunks) for p in (own[c], behind[c], ahead[c], *across[c])]
        send = pick(pieces, at)
        recv = [lax.all_to_all(send[e].reshape(ep, capacity, width), "ep", 0, 0, tiled=True) for e in range(count)]

        recv[0], pieces = lax.optimization_barrier((recv[0], pieces))

        lane = jnp.arange(experts, dtype=jnp.int32)
        probs = jax.nn.softmax(jnp.dot(jnp.concatenate(pieces), gate_w, preferred_element_type=F32), axis=-1)
        order = jnp.array([0, tp - 1, 1, 2], jnp.int32)
        seqs = (jnp.arange(chunks, dtype=jnp.int32)[:, None] * tp + (order + me) % tp).reshape(-1)
        both = []
        for idx in (idx_first, idx_second):
            turned = jnp.take(idx, seqs, axis=0).reshape(-1)
            both.append(jnp.sum(jnp.where(turned[:, None] == lane, probs, 0.0), axis=1))
        total = both[0] + both[1]
        inverse = jnp.array([0, 2, 3, 1], jnp.int32)
        spots = (jnp.arange(chunks, dtype=jnp.int32)[:, None] * tp + inverse[(jnp.arange(tp) - me) % tp]).reshape(-1)
        gates = [jnp.take((g / total).reshape(num_seqs, length), spots, axis=0).reshape(chunks, -1) for g in both]
        none = count * ep * capacity
        rows = []
        for n, idx in enumerate((first_idx, second_idx)):
            local = idx % held
            mine = (ranks[n] < capacity) & (local // count == me)
            row = (local % count) * (ep * capacity) + idx // held * capacity + ranks[n]
            rows.append((jnp.where(mine, row, none) * TILE).reshape(chunks, -1))

        index = (me * count).astype(jnp.int32)[None]
        returned = []
        for e in range(count):
            mine = [[(w, True)] for w in weights]
            a, b = far[e]
            across_w = [[(a[0], False)], [(b[0], False)], [(a[1], False), (b[1], False)]]
            near = [[[(w, False)] for w in ws] for ws in (from_behind[e][0], from_ahead[e][0])]
            if e:
                recv[e], y = lax.optimization_barrier((recv[e], y))
                returned.append(lax.all_to_all(y, "ep", 0, 0, tiled=True).reshape(ep * capacity, width))
            if e < count - 1:
                partial = expert(recv[e], [mine] + near, index + e, None, False)
                y = expert(recv[e], [across_w], index + e, partial, True)
            else:
                partial = expert(recv[e], [mine, across_w], index + e, None, False)
                for n, (ws, vs) in enumerate(zip(from_behind[e], from_ahead[e])):
                    both_w = [[(w, False), (v, False)] for w, v in zip(ws, vs)]
                    if n and returned:
                        partial, returned[-1] = lax.optimization_barrier((partial, returned[-1]))
                    partial = expert(recv[e], [both_w], index + e, partial, n == len(from_behind[e]) - 1)
                y = partial
        returned.append(lax.all_to_all(y, "ep", 0, 0, tiled=True).reshape(ep * capacity, width))

        order_rows = jnp.stack([(me + turn) % tp for turn in (0, tp - 1, 1, 2)]).astype(jnp.int32) * length
        out = (tokens, width)
        for c in range(chunks):
            part = combine([r[c] for r in rows], [g[c] for g in gates], *returned)
            mixed = lax.psum_scatter(part, "tp", scatter_dimension=0, tiled=True)
            r, u = attention(res[c], mixed, norm_gain[2], norm_gain[3], late_w, 4 * share, first_w, 1, heads, block)
            cuts = 1 if c < chunks - 1 else 2
            size = length // cuts
            plan, pieces = [], []
            for n in range(cuts):
                y = dense(u[n * size:(n + 1) * size], r[n * size:(n + 1) * size], late_w)
                low, high = send_up(y), send_back(y)
                arrived = [y, low, high, send_up(low[:size // 2]), send_back(high[size // 2:])]
                plan += [(turn, n * size + at) for turn, at in ((0, 0), (1, 0), (2, 0), (3, 0), (3, size // 2))]
                pieces += arrived
            out = place(tuple(plan), order_rows + c * tp * length, pieces, out)
        return out.reshape(num_seqs, length, width)

    return jax.shard_map(device_step, mesh=mesh, in_specs=in_specs, out_specs=row_spec, check_vma=False)
```
